32 devices in a mesh: lat: 4 (over y, x), lon: 8 (over z, core).
Axes of the slice: x: 2, y: 2, z: 4, core: 2. Of those that a mesh axis runs over, the one named last changes fastest.
Arguments:
- pressure: float32 [4, 30, 5120], P('lat', None, 'lon'), may hold values from -6 to 6
- velocity: float32 [4, 30, 7680], P('lat', None, 'lon'), may hold values from -6 to 6
- edge_cells: int32 [4, 2, 7680], P('lat', None, 'lon'), may hold values from 0 to 1663
- cell_edges: int32 [4, 3, 5120], P('lat', None, 'lon'), may hold values from 0 to 1983
- send_cells: int32 [4, 8, 1024], P('lat', None, 'lon'), may hold values from 0 to 639
- send_edges: int32 [4, 8, 1024], P('lat', None, 'lon'), may hold values from 0 to 959
- inv_dual: float32 [4, 7680], P('lat', 'lon'), may hold values from 0.5 to 2
- edge_weight: float32 [4, 3, 5120], P('lat', None, 'lon'), may hold values from -3 to 3
- sound_speed: float32 [4, 5120], P('lat', 'lon'), may hold values from 0.1 to 0.6
- coupling: float32 [4, 30, 5120], P('lat', None, 'lon'), may hold values from 0.1 to 2
Outputs:
- pressure_out: float32 [4, 30, 5120], P('lat', None, 'lon')
- velocity_out: float32 [4, 30, 7680], P('lat', None, 'lon')
The draws below stay inside these ranges and needn't reach their ends.
Inputs may be any that keep to these rules, and one draw needn't show every extreme that they name: `edge_cells`: positions below 640 are own cells; position 640 + r * 128 + j is slot j of the halo piece from the neighbour at offset number r. `cell_edges`: positions below 960 are own edges; position 960 + r * 128 + j is slot j of the edge halo piece from the neighbour at offset number r. `send_cells`: indices of own cells. `send_edges`: indices of own edges.
All inputs are finite; a program needn't handle non-finite values.
Results may differ from the reference program's by a relative error of at most 0.0001.
Values sent between devices are 32-bit elements; how exact they have to be, the bound alone decides.
A program may use at most 64 MiB of HBM per device.

```python
import math
import jax
import jax.numpy as jnp
from jax import lax

C_DEV = 640
E_DEV = 960
HALO = 128
NLEV = 30
NSUB = 3
CELLS_ROW = 5120
EDGES_ROW = 7680
SLOTS_ROW = 1024
N_LAT = 4
N_LON = 8


def with_ends(values, own_key, smallest, largest):
    spot = [jax.random.randint(jax.random.fold_in(own_key, axis), (), 0, length) for axis, length in enumerate(values.shape)]
    longest = values.shape.index(max(values.shape))
    neighbour = spot[:longest] + [(spot[longest] + 1) % values.shape[longest]] + spot[longest + 1:]
    return values.at[tuple(spot)].set(smallest).at[tuple(neighbour)].set(largest)


def block_levels(own_key, dims, cuts, low, top_value):
    factor_of, own = 1.0, jax.random.fold_in(own_key, 6)
    for dim, shards_of in cuts:
        heights = jnp.exp(jax.random.uniform(jax.random.fold_in(own, dim), (shards_of,), jnp.float32, low / len(cuts), top_value / len(cuts)))
        factor_of = factor_of * jnp.repeat(heights, dims[dim] // shards_of).reshape([-1 if axis == dim else 1 for axis in range(len(dims))])
    return factor_of


def normal_values(rng, extent, scale, bound, cuts=(), kind=jnp.bfloat16):
    values = scale * jax.random.normal(rng, extent, jnp.float32)
    if cuts:
        values = values * block_levels(rng, extent, cuts, -0.22, 0.18)
    return jnp.clip(values, -bound, bound).astype(kind)


def setup_inputs(seed: int = 0) -> dict:
    streams_of = jax.random.split(jax.random.key(seed), 11)
    return {
        "pressure": normal_values(streams_of[0], (N_LAT, NLEV, CELLS_ROW), 1.0, 6.0, ((0, 4), (2, 8)), jnp.float32),
        "velocity": normal_values(streams_of[1], (N_LAT, NLEV, EDGES_ROW), 1.0, 6.0, ((0, 4), (2, 8)), jnp.float32),
        "edge_cells": with_ends(jax.random.randint(streams_of[2], (N_LAT, 2, EDGES_ROW), 0, C_DEV + 8 * HALO), jax.random.fold_in(streams_of[2], 1), 0, (C_DEV + 8 * HALO) - 1).astype(jnp.int32),
        "cell_edges": with_ends(jax.random.randint(streams_of[3], (N_LAT, 3, CELLS_ROW), 0, E_DEV + 8 * HALO), jax.random.fold_in(streams_of[3], 1), 0, (E_DEV + 8 * HALO) - 1).astype(jnp.int32),
        "send_cells": with_ends(jax.random.randint(streams_of[4], (N_LAT, 8, SLOTS_ROW), 0, C_DEV), jax.random.fold_in(streams_of[4], 1), 0, C_DEV - 1).astype(jnp.int32),
        "send_edges": with_ends(jax.random.randint(streams_of[5], (N_LAT, 8, SLOTS_ROW), 0, E_DEV), jax.random.fold_in(streams_of[5], 1), 0, E_DEV - 1).astype(jnp.int32),
        "inv_dual": jnp.clip(jnp.exp(math.log(2.0) - 1.3862944 * jax.random.uniform(streams_of[6], (N_LAT, EDGES_ROW), jnp.float32) ** block_levels(streams_of[6], (N_LAT, EDGES_ROW), ((0, 4), (1, 8)), -0.2, 0.2)), 0.5, 2.0),
        "edge_weight": normal_values(streams_of[7], (N_LAT, 3, CELLS_ROW), 0.5, 3.0, ((0, 4), (2, 8)), jnp.float32),
        "sound_speed": jnp.clip(jnp.exp(math.log(0.6) - 1.7917595 * jax.random.uniform(streams_of[8], (N_LAT, CELLS_ROW), jnp.float32) ** block_levels(streams_of[8], (N_LAT, CELLS_ROW), ((0, 4), (1, 8)), -0.2, 0.2)), 0.1, 0.6),
        "coupling": jnp.clip(jnp.exp(math.log(2.0) - 2.9957323 * jax.random.uniform(streams_of[9], (N_LAT, NLEV, CELLS_ROW), jnp.float32) ** block_levels(streams_of[9], (N_LAT, NLEV, CELLS_ROW), ((0, 4), (2, 8)), -0.2, 0.2)), 0.1, 2.0),
    }


DIRECTIONS = ((-1, -1), (-1, 0), (-1, 1), (0, -1), (0, 1), (1, -1), (1, 0), (1, 1))
step_scale = 0.5


def position(offset):
    return DIRECTIONS.index(offset)


def edge_update(normal, extended, edge_cells, inv_dual):
    gradient = (jnp.take(extended, edge_cells[1], axis=1) - jnp.take(extended, edge_cells[0], axis=1)) * inv_dual[None, :]
    return normal - step_scale * gradient


def column_solve(right_side, coupling):
    levels = right_side.shape[0]
    ratios = []
    scaled = []
    for level_index in range(levels):
        if level_index < levels - 1:
            upper_term = -coupling[level_index]
        else:
            upper_term = 0.0 * coupling[0]
        if level_index == 0:
            divisor = 1.0 + coupling[0]
            current = right_side[0] / divisor
        else:
            lower_term = -coupling[level_index - 1]
            diagonal = 1.0 + coupling[level_index - 1] + coupling[level_index]
            divisor = diagonal - lower_term * ratios[-1]
            current = (right_side[level_index] - lower_term * scaled[-1]) / divisor
        ratios.append(upper_term / divisor)
        scaled.append(current)
    result = [scaled[-1]]
    for level_index in range(levels - 2, -1, -1):
        result.insert(0, scaled[level_index] - ratios[level_index] * result[0])
    return jnp.stack(result)


def cell_update(values, edges_ext, cell_edges, edge_weight, sound_speed, coupling):
    divergence = jnp.take(edges_ext, cell_edges[0], axis=1) * edge_weight[0][None, :]
    divergence = divergence + jnp.take(edges_ext, cell_edges[1], axis=1) * edge_weight[1][None, :]
    divergence = divergence + jnp.take(edges_ext, cell_edges[2], axis=1) * edge_weight[2][None, :]
    right_side = values - sound_speed[None, :] * divergence
    return column_solve(right_side, coupling)


def device_layout(array, width):
    if array.ndim == 2:
        return array.reshape(N_LAT, N_LON, width)
    return array.reshape(N_LAT, array.shape[1], N_LON, width).transpose(0, 2, 1, 3)


def global_layout(array):
    return array.transpose(0, 2, 1, 3).reshape(N_LAT, array.shape[2], N_LON * array.shape[3])


def take_pieces(source, indices):
    return jnp.take(source, indices, axis=1)


def reference_extend(source, send_list):
    taker = jax.vmap(jax.vmap(take_pieces))
    pieces = []
    for offset in DIRECTIONS:
        piece = taker(source, send_list[:, :, position((-offset[0], -offset[1]))])
        piece = jnp.roll(piece, -offset[1], axis=1)
        if offset[0] == 1:
            piece = jnp.concatenate([piece[1:], jnp.zeros_like(piece[:1])], axis=0)
        elif offset[0] == -1:
            piece = jnp.concatenate([jnp.zeros_like(piece[:1]), piece[:-1]], axis=0)
        pieces.append(piece)
    return jnp.concatenate([source] + pieces, axis=3)


def band_edges(operands):
    return jax.vmap(edge_update)(*operands)


def band_cells(operands):
    return jax.vmap(cell_update)(*operands)


def reference(pressure, velocity, edge_cells, cell_edges, send_cells, send_edges, inv_dual, edge_weight, sound_speed, coupling):
    values = device_layout(pressure, C_DEV)
    normal = device_layout(velocity, E_DEV)
    edge_pairs = device_layout(edge_cells, E_DEV)
    cell_sides = device_layout(cell_edges, C_DEV)
    cell_lists = device_layout(send_cells, HALO)
    edge_lists = device_layout(send_edges, HALO)
    inverse = device_layout(inv_dual, E_DEV)
    weights = device_layout(edge_weight, C_DEV)
    speeds = device_layout(sound_speed, C_DEV)
    couples = device_layout(coupling, C_DEV)
    for substep in range(NSUB):
        extended = reference_extend(values, cell_lists)
        normal = lax.map(band_edges, (normal, extended, edge_pairs, inverse))
        edges_ext = reference_extend(normal, edge_lists)
        values = lax.map(band_cells, (values, edges_ext, cell_sides, weights, speeds, couples))
    return global_layout(values), global_layout(normal)
```

```python
import jax
import jax.numpy as jnp
from jax import lax
from jax.experimental import pallas as pl
from jax.experimental.pallas import tpu as pltpu
from jax.sharding import PartitionSpec as P

NSUB = 3
OFFSETS = ((-1, -1), (-1, 0), (-1, 1), (0, -1), (0, 1), (1, -1), (1, 0), (1, 1))
ORDER = (3, 4, 1, 6, 0, 2, 5, 7)
GROUPS = ((0, 2), (2, 8))
SEND_ORDER = (0, 2, 5, 7, 1, 6, 3, 4)
step_scale = 0.5
MESH = pl.DeviceIdType.MESH
F32, BF16 = jnp.float32, jnp.bfloat16


def split(x):
    hi = x.astype(BF16)
    lo = (x - hi.astype(F32)).astype(BF16)
    return jnp.concatenate([hi, lo], axis=0)


def joined(y):
    half = y.shape[0] // 2
    return y[:half] + y[half:]


def dot(x, w):
    return jnp.dot(x, w, preferred_element_type=F32)


def round_up(n, m):
    return (n + m - 1) // m * m


def build(dst, row0, rows, lane0, plus, minus, base):
    chunk = 32
    width = plus.shape[1]

    def body(i, carry):
        key = lax.broadcasted_iota(jnp.int32, (chunk, width), 0) + (base + i * chunk)
        hot = jnp.where(key == plus, 1.0, 0.0)
        if minus is not None:
            hot = hot - jnp.where(key == minus, 1.0, 0.0)
        start = pl.multiple_of(row0 + i * chunk, chunk)
        dst[pl.ds(start, chunk), lane0 : lane0 + width] = hot.astype(BF16)
        return carry

    lax.fori_loop(0, rows // chunk, body, 0)


def kernel(
    n_lat, n_lon, nlev, cells, edges, halo,
    p_in, v_in, ec, ce, sc, se, inv_dual, weight, sound, coupling,
    p_out, v_out,
    pf, vf, s_cells, s_edges, a_mat, b_mat, p_send, v_send, p_halo, v_halo,
    t_inv, t_low, t_up, work,
    p_ss, p_rs, v_ss, v_rs,
):
    a, b = lax.axis_index("lat"), lax.axis_index("lon")
    ecols = vf.shape[1]
    below, above = a > 0, a < n_lat - 1

    def if_there(p, fn):
        if p == 0:
            fn()
        else:
            pl.when(below if p < 0 else above)(fn)

    def target(offset):
        return (a + offset[0], lax.rem(b + offset[1] + n_lon, n_lon))

    p_halo[...] = jnp.zeros_like(p_halo)
    v_halo[...] = jnp.zeros_like(v_halo)

    barrier = pltpu.get_barrier_semaphore()
    for lat_step in (0, -1, 1):
        def greet(lat_step=lat_step):
            for offset in OFFSETS:
                if offset[0] == lat_step:
                    pl.semaphore_signal(
                        barrier, inc=1, device_id=target(offset), device_id_type=MESH
                    )
        if_there(lat_step, greet)

    pf[nlev - nlev % 8 :, :] = jnp.zeros_like(pf[nlev - nlev % 8 :, :])
    pf[0:nlev, :] = p_in[0]
    vf[...] = jnp.zeros_like(vf)
    vf[0:nlev, 0:edges] = v_in[0]
    for member in range(8):
        build(s_cells, 0, cells, member * halo, sc[0, member : member + 1, :], None, 0)

    bands = (a + n_lat - 1) // n_lat + (2 * n_lat - 2 - a) // n_lat
    pl.semaphore_wait(barrier, 2 + 3 * bands)

    def copy(member, send, land, ss, rs):
        spot = ORDER.index(7 - member)
        return pltpu.make_async_remote_copy(
            src_ref=send.at[member], dst_ref=land.at[spot],
            send_sem=ss.at[member], recv_sem=rs.at[spot],
            device_id=target(OFFSETS[member]), device_id_type=MESH,
        )

    def launch(source, selector, send, land, ss, rs):
        pieces = joined(dot(source, selector[...]))
        for member in range(8):
            send[member] = pieces[:, member * halo : (member + 1) * halo]
        for member in SEND_ORDER:
            if_there(OFFSETS[member][0], lambda: copy(member, send, land, ss, rs).start())

    def arrive(lo, hi, send, land, ss, rs):
        for spot in range(lo, hi):
            slot = ORDER[spot]
            if_there(OFFSETS[slot][0], lambda: copy(7 - slot, send, land, ss, rs).wait_recv())
        return split(jnp.concatenate([land[spot] for spot in range(lo, hi)], axis=1))

    def retire(send, land, ss, rs):
        for member in range(8):
            if_there(OFFSETS[member][0], lambda: copy(member, send, land, ss, rs).wait_send())

    for substep in range(NSUB):
        source = split(pf[...])
        launch(source, s_cells, p_send, p_halo, p_ss, p_rs)
        if substep == 0:
            first, second = ec[0, 0:1, :], ec[0, 1:2, :]
            build(a_mat, 0, cells, 0, second, first, 0)
            for spot, slot in enumerate(ORDER):
                build(a_mat, cells + spot * halo, halo, 0, second, first, cells + slot * halo)
            for member in range(8):
                build(s_edges, 0, ecols, member * halo, se[0, member : member + 1, :], None, 0)
        gradient = dot(source, a_mat[0:cells, :])
        for lo, hi in GROUPS:
            got = arrive(lo, hi, p_send, p_halo, p_ss, p_rs)
            gradient += dot(got, a_mat[cells + lo * halo : cells + hi * halo, :])
        retire(p_send, p_halo, p_ss, p_rs)
        vf[:, 0:edges] = vf[:, 0:edges] - (step_scale * inv_dual[...]) * joined(gradient)

        source = split(vf[...])
        launch(source, s_edges, v_send, v_halo, v_ss, v_rs)
        if substep == 0:
            for j in range(3):
                wanted = ce[0, j : j + 1, :]
                build(b_mat, 0, ecols, j * cells, wanted, None, 0)
                for spot, slot in enumerate(ORDER):
                    build(b_mat, ecols + spot * halo, halo, j * cells, wanted, None, edges + slot * halo)
            ratio = inverse = None
            for level in range(nlev):
                here = coupling[0, level : level + 1, :]
                if level == 0:
                    divisor = 1.0 + here
                else:
                    lower = coupling[0, level - 1 : level, :]
                    divisor = 1.0 + lower + here + lower * ratio
                inverse = 1.0 / divisor
                ratio = -here * inverse
                t_inv[level : level + 1, :] = inverse
                t_up[level : level + 1, :] = ratio
                if level > 0:
                    t_low[level : level + 1, :] = lower * inverse
        taken = dot(source, b_mat[0:ecols, :])
        for lo, hi in GROUPS:
            got = arrive(lo, hi, v_send, v_halo, v_ss, v_rs)
            taken += dot(got, b_mat[ecols + lo * halo : ecols + hi * halo, :])
        retire(v_send, v_halo, v_ss, v_rs)
        taken = joined(taken)
        divergence = taken[:, 0:cells] * weight[0, 0:1, :]
        for j in (1, 2):
            divergence += taken[:, j * cells : (j + 1) * cells] * weight[0, j : j + 1, :]
        right = pf[...] - sound[...] * divergence
        work[0:nlev, :] = right[0:nlev] * t_inv[...]

        current = work[0:1, :]
        for level in range(1, nlev):
            current = work[level : level + 1, :] + t_low[level : level + 1, :] * current
            work[level : level + 1, :] = current
        pf[nlev - 1 : nlev, :] = current
        for level in range(nlev - 2, -1, -1):
            current = work[level : level + 1, :] - t_up[level : level + 1, :] * current
            pf[level : level + 1, :] = current

    p_out[0] = pf[0:nlev, :]
    v_out[0] = vf[0:nlev, 0:edges]


def on_device(*args):
    pressure, velocity, send_cells = args[0], args[1], args[4]
    n_lat, n_lon = lax.axis_size("lat"), lax.axis_size("lon")
    nlev, cells, edges = pressure.shape[1], pressure.shape[2], velocity.shape[2]
    halo = send_cells.shape[2]
    rows, ecols = round_up(nlev, 32), round_up(edges, 128)
    vmem = pl.BlockSpec(memory_space=pltpu.VMEM)
    dma8 = pltpu.SemaphoreType.DMA((8,))

    def body(*refs):
        kernel(n_lat, n_lon, nlev, cells, edges, halo, *refs)

    return tuple(pl.pallas_call(
        body,
        name="substeps",
        out_shape=(
            jax.ShapeDtypeStruct(pressure.shape, F32),
            jax.ShapeDtypeStruct(velocity.shape, F32),
        ),
        in_specs=[vmem] * len(args),
        out_specs=(vmem, vmem),
        scratch_shapes=[
            pltpu.VMEM((rows, cells), F32),
            pltpu.VMEM((rows, ecols), F32),
            pltpu.VMEM((cells, 8 * halo), BF16),
            pltpu.VMEM((ecols, 8 * halo), BF16),
            pltpu.VMEM((cells + 8 * halo, edges), BF16),
            pltpu.VMEM((ecols + 8 * halo, 3 * cells), BF16),
            pltpu.VMEM((8, rows, halo), F32),
            pltpu.VMEM((8, rows, halo), F32),
            pltpu.VMEM((8, rows, halo), F32),
            pltpu.VMEM((8, rows, halo), F32),
            pltpu.VMEM((nlev, cells), F32),
            pltpu.VMEM((nlev, cells), F32),
            pltpu.VMEM((nlev, cells), F32),
            pltpu.VMEM((rows, cells), F32),
            dma8, dma8, dma8, dma8,
        ],
        compiler_params=pltpu.CompilerParams(collective_id=0, has_side_effects=True, vmem_limit_bytes=40 * 1024 * 1024),
    )(*args))


def solution(mesh):
    band = P("lat", None, "lon")
    flat = P("lat", "lon")
    return jax.shard_map(
        on_device,
        mesh=mesh,
        in_specs=(band, band, band, band, band, band, flat, band, flat, band),
        out_specs=(band, band),
        check_vma=False,
    )
```

```python
import jax
import jax.numpy as jnp
from jax import lax
from jax.experimental import pallas as pl
from jax.experimental.pallas import tpu as pltpu
from jax.sharding import PartitionSpec as P

NSUB = 3
OFFSETS = ((-1, -1), (-1, 0), (-1, 1), (0, -1), (0, 1), (1, -1), (1, 0), (1, 1))
ORDER = (3, 4, 1, 6, 0, 2, 5, 7)
GROUPS = ((0, 2), (2, 8))
SEND_ORDER = (0, 2, 5, 7, 1, 6, 3, 4)
step_scale = 0.5
MESH = pl.DeviceIdType.MESH
F32 = jnp.float32


def round_up(n, m):
    return (n + m - 1) // m * m


LANES = 128


def tiles_of(ref, width):
    return [ref[:, k * LANES : (k + 1) * LANES] for k in range(width // LANES)]


def spread(index, own, padded):
    return jnp.where(index >= own, index + (padded - own), index)


def kernel(
    n_lat, n_lon, nlev, cells, edges, halo,
    p_in, v_in, ec, ce, sc, se, inv_dual, weight, sound, coupling,
    p_out, v_out,
    pf, vf, p_send, v_send, p_halo, v_halo,
    t_inv, t_low, t_up, work, grad, div,
    p_ss, p_rs, v_ss, v_rs,
):
    a, b = lax.axis_index("lat"), lax.axis_index("lon")
    ecols = vf.shape[1]
    below, above = a > 0, a < n_lat - 1

    def if_there(p, fn):
        if p == 0:
            fn()
        else:
            pl.when(below if p < 0 else above)(fn)

    def target(offset):
        return (a + offset[0], lax.rem(b + offset[1] + n_lon, n_lon))

    p_halo[...] = jnp.zeros_like(p_halo)
    v_halo[...] = jnp.zeros_like(v_halo)

    barrier = pltpu.get_barrier_semaphore()
    for lat_step in (0, -1, 1):
        def greet(lat_step=lat_step):
            for offset in OFFSETS:
                if offset[0] == lat_step:
                    pl.semaphore_signal(
                        barrier, inc=1, device_id=target(offset), device_id_type=MESH
                    )
        if_there(lat_step, greet)

    pf[nlev - nlev % 8 :, :] = jnp.zeros_like(pf[nlev - nlev % 8 :, :])
    pf[0:nlev, :] = p_in[0]
    vf[...] = jnp.zeros_like(vf)
    vf[0:nlev, 0:edges] = v_in[0]
    ccols = pf.shape[1]

    bands = (a + n_lat - 1) // n_lat + (2 * n_lat - 2 - a) // n_lat
    pl.semaphore_wait(barrier, 2 + 3 * bands)

    def copy(member, send, land, ss, rs):
        spot = ORDER.index(7 - member)
        return pltpu.make_async_remote_copy(
            src_ref=send.at[member], dst_ref=land.at[spot],
            send_sem=ss.at[member], recv_sem=rs.at[spot],
            device_id=target(OFFSETS[member]), device_id_type=MESH,
        )

    def launch(tiles, lists, send, land, ss, rs):
        for member in SEND_ORDER:
            send[member] = pick(tiles, range(len(tiles)), lists[0, member : member + 1, :])
            if_there(OFFSETS[member][0], lambda: copy(member, send, land, ss, rs).start())

    def arrive(spot, send, land, ss, rs):
        slot = ORDER[spot]
        if_there(OFFSETS[slot][0], lambda: copy(7 - slot, send, land, ss, rs).wait_recv())

    def retire(send, land, ss, rs):
        for member in range(8):
            if_there(OFFSETS[member][0], lambda: copy(member, send, land, ss, rs).wait_send())

    def add_gradient(tiles, firsts, fresh):
        for k in range(ecols // LANES):
            cols = slice(k * LANES, (k + 1) * LANES)
            taken = [
                pick(tiles, firsts, spread(padded(ec, r, k), cells, ccols)) for r in (0, 1)
            ]
            change = taken[1] - taken[0]
            grad[:, cols] = change if fresh else grad[:, cols] + change

    def add_divergence(tiles, firsts, fresh):
        for k in range(ccols // LANES):
            cols = slice(k * LANES, (k + 1) * LANES)
            total = None if fresh else div[:, cols]
            for j in range(3):
                index = spread(ce[0, j : j + 1, cols], edges, ecols)
                term = pick(tiles, firsts, index) * weight[0, j : j + 1, cols]
                total = term if total is None else total + term
            div[:, cols] = total

    def padded(ref, r, k):
        stop = min(ref.shape[2], (k + 1) * LANES)
        row = ref[0, r : r + 1, k * LANES : stop]
        short = (k + 1) * LANES - stop
        return jnp.pad(row, ((0, 0), (0, short))) if short else row

    def pick(tiles, firsts, index):
        shape = tiles[0].shape
        lane = jnp.broadcast_to(index & (LANES - 1), shape)
        tile = jnp.broadcast_to(index >> 7, shape)
        out = jnp.zeros(shape, F32)
        for values, first in zip(tiles, firsts):
            moved = jnp.take_along_axis(values, lane, axis=1, mode="promise_in_bounds")
            out = jnp.where(tile == first, moved, out)
        return out

    def columns_solved():
        ratio = None
        for level in range(nlev):
            here = coupling[0, level : level + 1, :]
            if level == 0:
                divisor = 1.0 + here
            else:
                lower = coupling[0, level - 1 : level, :]
                divisor = 1.0 + lower + here + lower * ratio
            inverse = 1.0 / divisor
            ratio = -here * inverse
            t_inv[level : level + 1, :] = inverse
            t_up[level : level + 1, :] = ratio
            if level > 0:
                t_low[level : level + 1, :] = lower * inverse

    for substep in range(NSUB):
        own = tiles_of(pf, ccols)
        launch(own, sc, p_send, p_halo, p_ss, p_rs)
        if substep == 0:
            columns_solved()
        add_gradient(own, range(len(own)), True)
        for lo, hi in GROUPS:
            for spot in range(lo, hi):
                arrive(spot, p_send, p_halo, p_ss, p_rs)
            add_gradient(
                [p_halo[spot] for spot in range(lo, hi)],
                [ccols // LANES + ORDER[spot] for spot in range(lo, hi)], False,
            )
        retire(p_send, p_halo, p_ss, p_rs)
        vf[:, 0:edges] = vf[:, 0:edges] - (step_scale * inv_dual[...]) * grad[:, 0:edges]

        own = tiles_of(vf, ecols)
        launch(own, se, v_send, v_halo, v_ss, v_rs)
        add_divergence(own, range(len(own)), True)
        for lo, hi in GROUPS:
            for spot in range(lo, hi):
                arrive(spot, v_send, v_halo, v_ss, v_rs)
            add_divergence(
                [v_halo[spot] for spot in range(lo, hi)],
                [ecols // LANES + ORDER[spot] for spot in range(lo, hi)], False,
            )
        retire(v_send, v_halo, v_ss, v_rs)
        right = pf[...] - sound[...] * div[...]
        work[0:nlev, :] = right[0:nlev] * t_inv[...]

        current = work[0:1, :]
        for level in range(1, nlev):
            current = work[level : level + 1, :] + t_low[level : level + 1, :] * current
            work[level : level + 1, :] = current
        pf[nlev - 1 : nlev, :] = current
        for level in range(nlev - 2, -1, -1):
            current = work[level : level + 1, :] - t_up[level : level + 1, :] * current
            pf[level : level + 1, :] = current

    p_out[0] = pf[0:nlev, :]
    v_out[0] = vf[0:nlev, 0:edges]


def on_device(*args):
    pressure, velocity, send_cells = args[0], args[1], args[4]
    n_lat, n_lon = lax.axis_size("lat"), lax.axis_size("lon")
    nlev, cells, edges = pressure.shape[1], pressure.shape[2], velocity.shape[2]
    halo = send_cells.shape[2]
    rows, ecols = round_up(nlev, 32), round_up(edges, 128)
    vmem = pl.BlockSpec(memory_space=pltpu.VMEM)
    dma8 = pltpu.SemaphoreType.DMA((8,))

    def body(*refs):
        kernel(n_lat, n_lon, nlev, cells, edges, halo, *refs)

    return tuple(pl.pallas_call(
        body,
        name="substeps",
        out_shape=(
            jax.ShapeDtypeStruct(pressure.shape, F32),
            jax.ShapeDtypeStruct(velocity.shape, F32),
        ),
        in_specs=[vmem] * len(args),
        out_specs=(vmem, vmem),
        scratch_shapes=[
            pltpu.VMEM((rows, cells), F32),
            pltpu.VMEM((rows, ecols), F32),
            pltpu.VMEM((8, rows, halo), F32),
            pltpu.VMEM((8, rows, halo), F32),
            pltpu.VMEM((8, rows, halo), F32),
            pltpu.VMEM((8, rows, halo), F32),
            pltpu.VMEM((nlev, cells), F32),
            pltpu.VMEM((nlev, cells), F32),
            pltpu.VMEM((nlev, cells), F32),
            pltpu.VMEM((rows, cells), F32),
            pltpu.VMEM((rows, ecols), F32),
            pltpu.VMEM((rows, cells), F32),
            dma8, dma8, dma8, dma8,
        ],
        compiler_params=pltpu.CompilerParams(collective_id=0, has_side_effects=True, vmem_limit_bytes=40 * 1024 * 1024),
    )(*args))


def solution(mesh):
    band = P("lat", None, "lon")
    flat = P("lat", "lon")
    return jax.shard_map(
        on_device,
        mesh=mesh,
        in_specs=(band, band, band, band, band, band, flat, band, flat, band),
        out_specs=(band, band),
        check_vma=False,
    )
```

```python
import jax
import jax.numpy as jnp
from jax import lax
from jax.experimental import pallas as pl
from jax.experimental.pallas import tpu as pltpu
from jax.sharding import PartitionSpec as P

NSUB = 3
OFFSETS = ((-1, -1), (-1, 0), (-1, 1), (0, -1), (0, 1), (1, -1), (1, 0), (1, 1))
LANES = 128
step_scale = 0.5
MESH = pl.DeviceIdType.MESH
F32 = jnp.float32


def round_up(n, m):
    return (n + m - 1) // m * m


def tiles_of(ref, width):
    return [ref[:, k * LANES : (k + 1) * LANES] for k in range(width // LANES)]


def spread(index, own, padded):
    return jnp.where(index >= own, index + (padded - own), index)


def member_of(p, q):
    return (1 + q, 3 + (q + 1) // 2, 6 + q)[p + 1]


def kernel(
    n_lat, n_lon, nlev, cells, edges, halo,
    p_hbm, v_hbm, ec_hbm, ce_hbm, sc_hbm, se_hbm, inv_hbm, weight_hbm, sound_hbm, coupling_hbm,
    p_out, v_out,
    p_row, v_row, ec, ce, sc, se, inv_dual, weight, sound, coupling,
    pf, vf, p_send, v_send, p_halo, v_halo,
    t_inv, t_low, t_up, work, grad, div,
    p_ss, p_rs, v_ss, v_rs, in_sem, out_sem,
):
    a, b = lax.axis_index("lat"), lax.axis_index("lon")
    ccols, ecols = pf.shape[1], vf.shape[1]
    below, above = a > 0, a < n_lat - 1
    far = 2 * ((2 * b) // n_lon) - 1
    near = -far
    sends = [(-1, far), (1, far), (0, far), (-1, 0), (1, 0), (-1, near), (1, near), (0, near)]
    arrivals = [[(0, near), (-1, 0), (1, 0)], [(-1, near), (1, near), (0, far)], [(-1, far), (1, far)]]

    def if_there(p, fn):
        if p == 0:
            fn()
        else:
            pl.when(below if p < 0 else above)(fn)

    def target(p, q):
        return (a + p, lax.rem(b + q + n_lon, n_lon))

    barrier = pltpu.get_barrier_semaphore()
    for lat_step in (-1, 1, 0):
        def greet(lat_step=lat_step):
            for offset in OFFSETS:
                if offset[0] == lat_step:
                    pl.semaphore_signal(
                        barrier, inc=1, device_id=target(*offset), device_id_type=MESH
                    )
        if_there(lat_step, greet)

    pairs = [
        (coupling_hbm, coupling), (p_hbm, p_row), (sc_hbm, sc), (ec_hbm, ec), (v_hbm, v_row),
        (inv_hbm, inv_dual), (se_hbm, se), (ce_hbm, ce), (weight_hbm, weight), (sound_hbm, sound),
    ]
    loads = [pltpu.make_async_copy(x, y, in_sem.at[k]) for k, (x, y) in enumerate(pairs)]
    for load in loads:
        load.start()

    def clear(p):
        def fill():
            for slot, offset in enumerate(OFFSETS):
                if offset[0] == p:
                    p_halo[slot] = jnp.zeros(p_halo.shape[1:], F32)
                    v_halo[slot] = jnp.zeros(v_halo.shape[1:], F32)
        return fill

    pl.when(a == 0)(clear(-1))
    pl.when(a == n_lat - 1)(clear(1))
    pf[nlev - nlev % 8 :, :] = jnp.zeros_like(pf[nlev - nlev % 8 :, :])
    vf[...] = jnp.zeros_like(vf)

    def copy(p, q, send, land, ss, rs):
        member = member_of(p, q)
        return pltpu.make_async_remote_copy(
            src_ref=send.at[member], dst_ref=land.at[7 - member],
            send_sem=ss.at[member], recv_sem=rs.at[7 - member],
            device_id=target(p, q), device_id_type=MESH,
        )

    def collect(tiles, lists, send, offsets):
        for p, q in offsets:
            index = lists[0, pl.ds(member_of(p, q), 1), :]
            send[member_of(p, q)] = pick(tiles, range(len(tiles)), index)

    def launch(offsets, *refs):
        for p, q in offsets:
            if_there(p, lambda: copy(p, q, *refs).start())

    def arrive(group, *refs):
        for p, q in group:
            if_there(p, lambda: copy(-p, -q, *refs).wait_recv())

    def retire(*refs):
        for p, q in sends:
            if_there(p, lambda: copy(p, q, *refs).wait_send())

    def pick(tiles, firsts, index):
        shape = tiles[0].shape
        lane = jnp.broadcast_to(index & (LANES - 1), shape)
        tile = jnp.broadcast_to(index >> 7, shape)
        out = jnp.zeros(shape, F32)
        for values, first in zip(tiles, firsts):
            moved = jnp.take_along_axis(values, lane, axis=1, mode="promise_in_bounds")
            out = jnp.where(tile == first, moved, out)
        return out

    def halo_tiles(land, group, own):
        slots = [member_of(p, q) for p, q in group]
        return [land[slot] for slot in slots], [own + slot for slot in slots]

    def edge_columns(ref, row, k):
        stop = min(edges, (k + 1) * LANES)
        part = row(ref)[:, k * LANES : stop]
        short = (k + 1) * LANES - stop
        return jnp.pad(part, ((0, 0), (0, short))) if short else part

    def add_gradient(tiles, firsts, fresh, last):
        for k in range(ecols // LANES):
            cols = slice(k * LANES, (k + 1) * LANES)
            taken = [
                pick(tiles, firsts, spread(edge_columns(ec, lambda ref: ref[0, r : r + 1, :], k), cells, ccols))
                for r in (0, 1)
            ]
            change = taken[1] - taken[0]
            total = change if fresh else grad[:, cols] + change
            if last:
                scale = step_scale * edge_columns(inv_dual, lambda ref: ref[...], k)
                vf[:, cols] = vf[:, cols] - scale * total
            else:
                grad[:, cols] = total

    def add_divergence(tiles, firsts, fresh, last):
        for k in range(ccols // LANES):
            cols = slice(k * LANES, (k + 1) * LANES)
            total = None if fresh else div[:, cols]
            for j in range(3):
                term = pick(tiles, firsts, spread(ce[j, :, cols], edges, ecols)) * weight[j, :, cols]
                total = term if total is None else total + term
            if last:
                right = pf[:, cols] - sound[:, cols] * total
                work[0:nlev, cols] = right[0:nlev] * t_inv[:, cols]
            else:
                div[:, cols] = total

    def columns_solved():
        ratio = None
        for level in range(nlev):
            here = coupling[level]
            if level == 0:
                divisor = 1.0 + here
            else:
                lower = coupling[level - 1]
                divisor = 1.0 + lower + here + lower * ratio
            inverse = 1.0 / divisor
            ratio = -here * inverse
            t_inv[level : level + 1, :] = inverse
            t_up[level : level + 1, :] = ratio
            if level > 0:
                t_low[level : level + 1, :] = lower * inverse

    p_refs = (p_send, p_halo, p_ss, p_rs)
    v_refs = (v_send, v_halo, v_ss, v_rs)
    for load in loads[:3]:
        load.wait()
    for level in range(nlev):
        pf[level : level + 1, :] = p_row[level]
    own = tiles_of(pf, ccols)
    collect(own, sc, p_send, sends)
    columns_solved()
    bands = (a + n_lat - 1) // n_lat + (2 * n_lat - 2 - a) // n_lat
    pl.semaphore_wait(barrier, 2 + 3 * bands)

    for substep in range(NSUB):
        final = substep == NSUB - 1
        if substep == 0:
            launch(sends, *p_refs)
            for load in loads[3:]:
                load.wait()
            for level in range(nlev):
                vf[level : level + 1, 0:edges] = v_row[level]
        else:
            own = tiles_of(pf, ccols)
            for part in (sends[:3], sends[3:]):
                collect(own, sc, p_send, part)
                launch(part, *p_refs)
        add_gradient(own, range(len(own)), True, False)
        for k, group in enumerate(arrivals):
            arrive(group, *p_refs)
            add_gradient(*halo_tiles(p_halo, group, ccols // LANES), False, k == 2)
        retire(*p_refs)

        own = tiles_of(vf, ecols)
        for part in (sends[:3], sends[3:]):
            collect(own, se, v_send, part)
            launch(part, *v_refs)
        if final:
            for level in range(nlev):
                v_row[level] = vf[level : level + 1, 0:edges]
            v_store = pltpu.make_async_copy(v_row, v_out, out_sem.at[0])
            v_store.start()
        add_divergence(own, range(len(own)), True, False)
        for k, group in enumerate(arrivals):
            arrive(group, *v_refs)
            add_divergence(*halo_tiles(v_halo, group, ecols // LANES), False, k == 2)
        retire(*v_refs)

        current = work[0:1, :]
        for level in range(1, nlev):
            current = work[level : level + 1, :] + t_low[level : level + 1, :] * current
            work[level : level + 1, :] = current
        for level in range(nlev - 1, -1, -1):
            if level < nlev - 1:
                current = work[level : level + 1, :] - t_up[level : level + 1, :] * current
            if final:
                p_row[level] = current
            else:
                pf[level : level + 1, :] = current

    p_store = pltpu.make_async_copy(p_row, p_out, out_sem.at[1])
    p_store.start()
    p_store.wait()
    v_store.wait()


def level_major(x):
    return jnp.transpose(x, (1, 0, 2))


def on_device(*args):
    pressure, velocity, send_cells = args[0], args[1], args[4]
    n_lat, n_lon = lax.axis_size("lat"), lax.axis_size("lon")
    nlev, cells, edges = pressure.shape[1], pressure.shape[2], velocity.shape[2]
    halo = send_cells.shape[2]
    rows, ecols = round_up(nlev, 32), round_up(edges, 128)
    hbm = pl.BlockSpec(memory_space=pltpu.HBM)
    dma8 = pltpu.SemaphoreType.DMA((8,))
    args = [level_major(x) if k in (0, 1, 3, 7, 9) else x for k, x in enumerate(args)]

    def body(*refs):
        kernel(n_lat, n_lon, nlev, cells, edges, halo, *refs)

    halo_shape = pltpu.VMEM((8, rows, halo), F32)
    cell_shape = pltpu.VMEM((rows, cells), F32)
    edge_shape = pltpu.VMEM((rows, ecols), F32)
    level_shape = pltpu.VMEM((nlev, cells), F32)
    outs = pl.pallas_call(
        body,
        name="substeps",
        out_shape=(
            jax.ShapeDtypeStruct(args[0].shape, F32),
            jax.ShapeDtypeStruct(args[1].shape, F32),
        ),
        in_specs=[hbm] * len(args),
        out_specs=(hbm, hbm),
        scratch_shapes=[pltpu.VMEM(x.shape, x.dtype) for x in args] + [
            cell_shape, edge_shape, halo_shape, halo_shape, halo_shape, halo_shape,
            level_shape, level_shape, level_shape, cell_shape, edge_shape, cell_shape,
            dma8, dma8, dma8, dma8,
            pltpu.SemaphoreType.DMA((len(args),)), pltpu.SemaphoreType.DMA((2,)),
        ],
        compiler_params=pltpu.CompilerParams(
            collective_id=0, has_side_effects=True, vmem_limit_bytes=67_000_000
        ),
    )(*args)
    return tuple(level_major(x) for x in outs)


def solution(mesh):
    band = P("lat", None, "lon")
    flat = P("lat", "lon")
    return jax.shard_map(
        on_device,
        mesh=mesh,
        in_specs=(band, band, band, band, band, band, flat, band, flat, band),
        out_specs=(band, band),
        check_vma=False,
    )
```

```python
import jax
import jax.numpy as jnp
from jax import lax
from jax.experimental import pallas as pl
from jax.experimental.pallas import tpu as pltpu
from jax.sharding import PartitionSpec as P

NSUB = 3
OFFSETS = ((-1, -1), (-1, 0), (-1, 1), (0, -1), (0, 1), (1, -1), (1, 0), (1, 1))
LANES = 128
step_scale = 0.5
MESH = pl.DeviceIdType.MESH
F32 = jnp.float32


def round_up(n, m):
    return (n + m - 1) // m * m


def tiles_of(ref, width):
    return [ref[:, k * LANES : (k + 1) * LANES] for k in range(width // LANES)]


def spread(index, own, padded):
    return jnp.where(index >= own, index + (padded - own), index)


def member_of(p, q):
    return (1 + q, 3 + (q + 1) // 2, 6 + q)[p + 1]


def kernel(
    n_lat, n_lon, nlev, cells, edges, halo,
    p_hbm, v_hbm, ec_hbm, ce_hbm, sc_hbm, se_hbm, inv_hbm, weight_hbm, sound_hbm, coupling_hbm,
    p_out, v_out,
    p_row, v_row, ec, ce, sc, se, inv_dual, weight, sound, coupling,
    pf, vf, p_send, v_send, p_halo, v_halo,
    t_inv, t_low, t_up, work, grad, div,
    p_ss, p_rs, v_ss, v_rs, in_sem,
):
    a, b = lax.axis_index("lat"), lax.axis_index("lon")
    ccols, ecols = pf.shape[1], vf.shape[1]
    below, above = a > 0, a < n_lat - 1
    far = 2 * ((2 * b) // n_lon) - 1
    near = -far
    sends = [(-1, far), (1, far), (0, far), (-1, 0), (1, 0), (-1, near), (1, near), (0, near)]
    arrivals = [[(0, near), (-1, 0), (1, 0), (-1, near), (1, near), (0, far)], [(-1, far), (1, far)]]

    def if_there(p, fn):
        if p == 0:
            fn()
        else:
            pl.when(below if p < 0 else above)(fn)

    def target(p, q):
        return (a + p, lax.rem(b + q + n_lon, n_lon))

    barrier = pltpu.get_barrier_semaphore()
    for lat_step in (-1, 1, 0):
        def greet(lat_step=lat_step):
            for offset in OFFSETS:
                if offset[0] == lat_step:
                    pl.semaphore_signal(
                        barrier, inc=1, device_id=target(*offset), device_id_type=MESH
                    )
        if_there(lat_step, greet)

    pairs = [
        (coupling_hbm, coupling), (p_hbm, p_row), (sc_hbm, sc), (ec_hbm, ec), (v_hbm, v_row),
        (inv_hbm, inv_dual), (se_hbm, se), (ce_hbm, ce), (weight_hbm, weight), (sound_hbm, sound),
    ]
    loads = [pltpu.make_async_copy(x, y, in_sem.at[k]) for k, (x, y) in enumerate(pairs)]
    for load in loads:
        load.start()

    def clear(p):
        def fill():
            for slot, offset in enumerate(OFFSETS):
                if offset[0] == p:
                    p_halo[slot] = jnp.zeros(p_halo.shape[1:], F32)
                    v_halo[slot] = jnp.zeros(v_halo.shape[1:], F32)
        return fill

    pl.when(a == 0)(clear(-1))
    pl.when(a == n_lat - 1)(clear(1))
    pf[nlev - nlev % 8 :, :] = jnp.zeros_like(pf[nlev - nlev % 8 :, :])
    vf[...] = jnp.zeros_like(vf)

    def copy(p, q, send, land, ss, rs):
        member = member_of(p, q)
        return pltpu.make_async_remote_copy(
            src_ref=send.at[member], dst_ref=land.at[7 - member],
            send_sem=ss.at[member], recv_sem=rs.at[7 - member],
            device_id=target(p, q), device_id_type=MESH,
        )

    def collect(tiles, lists, send, offsets):
        for p, q in offsets:
            index = lists[0, pl.ds(member_of(p, q), 1), :]
            send[member_of(p, q)] = pick(tiles, range(len(tiles)), index)

    def launch(offsets, *refs):
        for p, q in offsets:
            if_there(p, lambda: copy(p, q, *refs).start())

    def arrive(group, *refs):
        for p, q in group:
            if_there(p, lambda: copy(-p, -q, *refs).wait_recv())

    def retire(*refs):
        for p, q in sends:
            if_there(p, lambda: copy(p, q, *refs).wait_send())

    def pick(tiles, firsts, index):
        shape = tiles[0].shape
        lane = jnp.broadcast_to(index & (LANES - 1), shape)
        tile = jnp.broadcast_to(index >> 7, shape)
        out = jnp.zeros(shape, F32)
        for values, first in zip(tiles, firsts):
            moved = jnp.take_along_axis(values, lane, axis=1, mode="promise_in_bounds")
            out = jnp.where(tile == first, moved, out)
        return out

    def halo_tiles(land, group, own):
        slots = [member_of(p, q) for p, q in group]
        return [land[slot] for slot in slots], [own + slot for slot in slots]

    def edge_columns(ref, row, k):
        stop = min(edges, (k + 1) * LANES)
        part = row(ref)[:, k * LANES : stop]
        short = (k + 1) * LANES - stop
        return jnp.pad(part, ((0, 0), (0, short))) if short else part

    def add_gradient(tiles, firsts, fresh, last):
        for k in range(ecols // LANES):
            cols = slice(k * LANES, (k + 1) * LANES)
            taken = [
                pick(tiles, firsts, spread(edge_columns(ec, lambda ref: ref[0, r : r + 1, :], k), cells, ccols))
                for r in (0, 1)
            ]
            change = taken[1] - taken[0]
            total = change if fresh else grad[:, cols] + change
            if last:
                scale = step_scale * edge_columns(inv_dual, lambda ref: ref[...], k)
                vf[:, cols] = vf[:, cols] - scale * total
            else:
                grad[:, cols] = total

    def add_divergence(tiles, firsts, fresh, last):
        for k in range(ccols // LANES):
            cols = slice(k * LANES, (k + 1) * LANES)
            total = None if fresh else div[:, cols]
            for j in range(3):
                term = pick(tiles, firsts, spread(ce[j, :, cols], edges, ecols)) * weight[j, :, cols]
                total = term if total is None else total + term
            if last:
                right = pf[:, cols] - sound[:, cols] * total
                work[0:nlev, cols] = right[0:nlev] * t_inv[:, cols]
            else:
                div[:, cols] = total

    def columns_solved():
        ratio = None
        for level in range(nlev):
            here = coupling[level]
            if level == 0:
                divisor = 1.0 + here
            else:
                lower = coupling[level - 1]
                divisor = 1.0 + lower + here + lower * ratio
            inverse = 1.0 / divisor
            ratio = -here * inverse
            t_inv[level : level + 1, :] = inverse
            t_up[level : level + 1, :] = ratio
            if level > 0:
                t_low[level : level + 1, :] = lower * inverse

    p_refs = (p_send, p_halo, p_ss, p_rs)
    v_refs = (v_send, v_halo, v_ss, v_rs)
    for load in loads[:3]:
        load.wait()
    for level in range(nlev):
        pf[level : level + 1, :] = p_row[level]
    own = tiles_of(pf, ccols)
    collect(own, sc, p_send, sends)
    columns_solved()
    bands = (a + n_lat - 1) // n_lat + (2 * n_lat - 2 - a) // n_lat
    pl.semaphore_wait(barrier, 2 + 3 * bands)

    for substep in range(NSUB):
        final = substep == NSUB - 1
        if substep == 0:
            launch(sends, *p_refs)
            for load in loads[3:]:
                load.wait()
            for level in range(nlev):
                vf[level : level + 1, 0:edges] = v_row[level]
        else:
            own = tiles_of(pf, ccols)
            for part in (sends[:3], sends[3:]):
                collect(own, sc, p_send, part)
                launch(part, *p_refs)
        add_gradient(own, range(len(own)), True, False)
        for k, group in enumerate(arrivals):
            arrive(group, *p_refs)
            add_gradient(*halo_tiles(p_halo, group, ccols // LANES), False, k == 1)
        retire(*p_refs)

        own = tiles_of(vf, ecols)
        for part in (sends[:3], sends[3:]):
            collect(own, se, v_send, part)
            launch(part, *v_refs)
        if final:
            for level in range(nlev):
                v_out[level] = vf[level : level + 1, 0:edges]
        add_divergence(own, range(len(own)), True, False)
        for k, group in enumerate(arrivals):
            arrive(group, *v_refs)
            add_divergence(*halo_tiles(v_halo, group, ecols // LANES), False, k == 1)
        retire(*v_refs)

        current = work[0:1, :]
        for level in range(1, nlev):
            current = work[level : level + 1, :] + t_low[level : level + 1, :] * current
            work[level : level + 1, :] = current
        for level in range(nlev - 1, -1, -1):
            if level < nlev - 1:
                current = work[level : level + 1, :] - t_up[level : level + 1, :] * current
            if final:
                p_out[level] = current
            else:
                pf[level : level + 1, :] = current


def write_out(p_ref, v_ref, p_out, v_out, sem):
    stores = [
        pltpu.make_async_copy(x, y, sem.at[k])
        for k, (x, y) in enumerate(((v_ref, v_out), (p_ref, p_out)))
    ]
    for store in stores:
        store.start()
    for store in stores:
        store.wait()


def level_major(x):
    return jnp.transpose(x, (1, 0, 2))


def on_device(*args):
    pressure, velocity, send_cells = args[0], args[1], args[4]
    n_lat, n_lon = lax.axis_size("lat"), lax.axis_size("lon")
    nlev, cells, edges = pressure.shape[1], pressure.shape[2], velocity.shape[2]
    halo = send_cells.shape[2]
    rows, ecols = round_up(nlev, 32), round_up(edges, 128)
    hbm = pl.BlockSpec(memory_space=pltpu.HBM)
    vmem = pl.BlockSpec(memory_space=pltpu.VMEM)
    dma8 = pltpu.SemaphoreType.DMA((8,))
    args = [level_major(x) if k in (0, 1, 3, 7, 9) else x for k, x in enumerate(args)]

    def body(*refs):
        kernel(n_lat, n_lon, nlev, cells, edges, halo, *refs)

    halo_shape = pltpu.VMEM((8, rows, halo), F32)
    cell_shape = pltpu.VMEM((rows, cells), F32)
    edge_shape = pltpu.VMEM((rows, ecols), F32)
    level_shape = pltpu.VMEM((nlev, cells), F32)
    outs = pl.pallas_call(
        body,
        name="substeps",
        out_shape=(
            pltpu.VMEM(args[0].shape, F32),
            pltpu.VMEM(args[1].shape, F32),
        ),
        in_specs=[hbm] * len(args),
        out_specs=(vmem, vmem),
        scratch_shapes=[pltpu.VMEM(x.shape, x.dtype) for x in args] + [
            cell_shape, edge_shape, halo_shape, halo_shape, halo_shape, halo_shape,
            level_shape, level_shape, level_shape, cell_shape, edge_shape, cell_shape,
            dma8, dma8, dma8, dma8,
            pltpu.SemaphoreType.DMA((len(args),)),
        ],
        compiler_params=pltpu.CompilerParams(
            collective_id=0, has_side_effects=True, vmem_limit_bytes=66_000_000
        ),
    )(*args)
    outs = pl.pallas_call(
        write_out,
        name="write_out",
        out_shape=tuple(jax.ShapeDtypeStruct(x.shape, F32) for x in outs),
        in_specs=[vmem] * 2,
        out_specs=(hbm, hbm),
        scratch_shapes=[pltpu.SemaphoreType.DMA((2,))],
        compiler_params=pltpu.CompilerParams(vmem_limit_bytes=1024 * 1024),
    )(*outs)
    return tuple(level_major(x) for x in outs)


def solution(mesh):
    band = P("lat", None, "lon")
    flat = P("lat", "lon")
    return jax.shard_map(
        on_device,
        mesh=mesh,
        in_specs=(band, band, band, band, band, band, flat, band, flat, band),
        out_specs=(band, band),
        check_vma=False,
    )
```

```python
import jax
import jax.numpy as jnp
from jax import lax
from jax.experimental import pallas as pl
from jax.experimental.pallas import tpu as pltpu
from jax.sharding import PartitionSpec as P

NSUB = 3
OFFSETS = ((-1, -1), (-1, 0), (-1, 1), (0, -1), (0, 1), (1, -1), (1, 0), (1, 1))
LANES = 128
step_scale = 0.5
MESH = pl.DeviceIdType.MESH
F32 = jnp.float32


def round_up(n, m):
    return (n + m - 1) // m * m


def tiles_of(ref, width):
    return [ref[:, k * LANES : (k + 1) * LANES] for k in range(width // LANES)]


def spread(index, own, padded):
    return jnp.where(index >= own, index + (padded - own), index)


def member_of(p, q):
    return (1 + q, 3 + (q + 1) // 2, 6 + q)[p + 1]


def kernel(
    n_lat, n_lon, nlev, cells, edges, halo,
    p_hbm, v_hbm, ec_hbm, ce_hbm, sc_hbm, se_hbm, inv_hbm, weight_hbm, sound_hbm, coupling_hbm,
    p_out, v_out,
    p_row, v_row, ec, ce, sc, se, inv_dual, weight, sound, coupling,
    pf, vf, p_send, v_send, p_halo, v_halo,
    t_inv, t_low, t_up, work, grad, div,
    p_ss, p_rs, v_ss, v_rs, in_sem,
):
    a, b = lax.axis_index("lat"), lax.axis_index("lon")
    ccols, ecols = pf.shape[1], vf.shape[1]
    below, above = a > 0, a < n_lat - 1
    far = 2 * ((2 * b) // n_lon) - 1
    near = -far
    sends = [(-1, far), (1, far), (0, far), (-1, 0), (1, 0), (-1, near), (1, near), (0, near)]
    arrivals = [[(0, near), (-1, 0), (1, 0), (-1, near), (1, near), (0, far)], [(-1, far), (1, far)]]

    def if_there(p, fn):
        if p == 0:
            fn()
        else:
            pl.when(below if p < 0 else above)(fn)

    def target(p, q):
        return (a + p, lax.rem(b + q + n_lon, n_lon))

    barrier = pltpu.get_barrier_semaphore()
    for lat_step in (-1, 1, 0):
        def greet(lat_step=lat_step):
            for offset in OFFSETS:
                if offset[0] == lat_step:
                    pl.semaphore_signal(
                        barrier, inc=1, device_id=target(*offset), device_id_type=MESH
                    )
        if_there(lat_step, greet)

    pairs = [
        (coupling_hbm, coupling), (p_hbm, p_row), (sc_hbm, sc), (ec_hbm, ec), (v_hbm, v_row),
        (inv_hbm, inv_dual), (se_hbm, se), (ce_hbm, ce), (weight_hbm, weight), (sound_hbm, sound),
    ]
    loads = [pltpu.make_async_copy(x, y, in_sem.at[k]) for k, (x, y) in enumerate(pairs)]
    for load in loads:
        load.start()

    def clear(p):
        def fill():
            for slot, offset in enumerate(OFFSETS):
                if offset[0] == p:
                    p_halo[slot] = jnp.zeros(p_halo.shape[1:], F32)
                    v_halo[slot] = jnp.zeros(v_halo.shape[1:], F32)
        return fill

    pl.when(a == 0)(clear(-1))
    pl.when(a == n_lat - 1)(clear(1))
    pf[nlev - nlev % 8 :, :] = jnp.zeros_like(pf[nlev - nlev % 8 :, :])
    vf[...] = jnp.zeros_like(vf)

    def copy(p, q, send, land, ss, rs):
        member = member_of(p, q)
        return pltpu.make_async_remote_copy(
            src_ref=send.at[member], dst_ref=land.at[7 - member],
            send_sem=ss.at[member], recv_sem=rs.at[7 - member],
            device_id=target(p, q), device_id_type=MESH,
        )

    def collect(tiles, lists, send, offsets):
        for p, q in offsets:
            index = lists[0, pl.ds(member_of(p, q), 1), :]
            send[member_of(p, q)] = pick(tiles, range(len(tiles)), index)

    def launch(offsets, *refs):
        for p, q in offsets:
            if_there(p, lambda: copy(p, q, *refs).start())

    def arrive(group, *refs):
        for p, q in group:
            if_there(p, lambda: copy(-p, -q, *refs).wait_recv())

    def retire(*refs):
        for p, q in sends:
            if_there(p, lambda: copy(p, q, *refs).wait_send())

    def pick(tiles, firsts, index):
        shape = tiles[0].shape
        lane = jnp.broadcast_to(index & (LANES - 1), shape)
        tile = jnp.broadcast_to(index >> 7, shape)
        out = jnp.zeros(shape, F32)
        for values, first in zip(tiles, firsts):
            moved = jnp.take_along_axis(values, lane, axis=1, mode="promise_in_bounds")
            out = jnp.where(tile == first, moved, out)
        return out

    def halo_tiles(land, group, own):
        slots = [member_of(p, q) for p, q in group]
        return [land[slot] for slot in slots], [own + slot for slot in slots]

    def edge_columns(ref, row, k):
        stop = min(edges, (k + 1) * LANES)
        part = row(ref)[:, k * LANES : stop]
        short = (k + 1) * LANES - stop
        return jnp.pad(part, ((0, 0), (0, short))) if short else part

    def add_gradient(tiles, firsts, fresh, last):
        for k in range(ecols // LANES):
            cols = slice(k * LANES, (k + 1) * LANES)
            taken = [
                pick(tiles, firsts, spread(edge_columns(ec, lambda ref: ref[0, r : r + 1, :], k), cells, ccols))
                for r in (0, 1)
            ]
            change = taken[1] - taken[0]
            total = change if fresh else grad[:, cols] + change
            if last:
                scale = step_scale * edge_columns(inv_dual, lambda ref: ref[...], k)
                vf[:, cols] = vf[:, cols] - scale * total
            else:
                grad[:, cols] = total

    def add_divergence(tiles, firsts, fresh, last):
        for k in range(ccols // LANES):
            cols = slice(k * LANES, (k + 1) * LANES)
            total = None if fresh else div[:, cols]
            for j in range(3):
                term = pick(tiles, firsts, spread(ce[j, :, cols], edges, ecols)) * weight[j, :, cols]
                total = term if total is None else total + term
            if last:
                right = pf[:, cols] - sound[:, cols] * total
                work[0:nlev, cols] = right[0:nlev] * t_inv[:, cols]
            else:
                div[:, cols] = total

    def columns_solved():
        ratio = None
        for level in range(nlev):
            here = coupling[level]
            if level == 0:
                divisor = 1.0 + here
            else:
                lower = coupling[level - 1]
                divisor = 1.0 + lower + here + lower * ratio
            inverse = 1.0 / divisor
            ratio = -here * inverse
            t_inv[level : level + 1, :] = inverse
            t_up[level : level + 1, :] = ratio
            if level > 0:
                t_low[level : level + 1, :] = lower * inverse

    p_refs = (p_send, p_halo, p_ss, p_rs)
    v_refs = (v_send, v_halo, v_ss, v_rs)
    for load in loads[:3]:
        load.wait()
    for level in range(nlev):
        pf[level : level + 1, :] = p_row[level]
    own = tiles_of(pf, ccols)
    collect(own, sc, p_send, sends)
    columns_solved()
    bands = (a + n_lat - 1) // n_lat + (2 * n_lat - 2 - a) // n_lat
    pl.semaphore_wait(barrier, 2 + 3 * bands)

    for substep in range(NSUB):
        final = substep == NSUB - 1
        if substep == 0:
            launch(sends, *p_refs)
            for load in loads[3:]:
                load.wait()
            for level in range(nlev):
                vf[level : level + 1, 0:edges] = v_row[level]
        else:
            own = tiles_of(pf, ccols)
            for part in (sends[:3], sends[3:]):
                collect(own, sc, p_send, part)
                launch(part, *p_refs)
        add_gradient(own, range(len(own)), True, False)
        if substep > 0:
            retire(*v_refs)
        for k, group in enumerate(arrivals):
            arrive(group, *p_refs)
            add_gradient(*halo_tiles(p_halo, group, ccols // LANES), False, k == 1)

        own = tiles_of(vf, ecols)
        for part in (sends[:3], sends[3:]):
            collect(own, se, v_send, part)
            launch(part, *v_refs)
        if final:
            for level in range(nlev):
                v_out[level] = vf[level : level + 1, 0:edges]
        add_divergence(own, range(len(own)), True, False)
        retire(*p_refs)
        for k, group in enumerate(arrivals):
            arrive(group, *v_refs)
            add_divergence(*halo_tiles(v_halo, group, ecols // LANES), False, k == 1)

        current = work[0:1, :]
        for level in range(1, nlev):
            current = work[level : level + 1, :] + t_low[level : level + 1, :] * current
            work[level : level + 1, :] = current
        for level in range(nlev - 1, -1, -1):
            if level < nlev - 1:
                current = work[level : level + 1, :] - t_up[level : level + 1, :] * current
            if final:
                p_out[level] = current
            else:
                pf[level : level + 1, :] = current

    retire(*v_refs)


def write_out(p_ref, v_ref, p_out, v_out, sem):
    stores = [
        pltpu.make_async_copy(x, y, sem.at[k])
        for k, (x, y) in enumerate(((v_ref, v_out), (p_ref, p_out)))
    ]
    for store in stores:
        store.start()
    for store in stores:
        store.wait()


def level_major(x):
    return jnp.transpose(x, (1, 0, 2))


def on_device(*args):
    pressure, velocity, send_cells = args[0], args[1], args[4]
    n_lat, n_lon = lax.axis_size("lat"), lax.axis_size("lon")
    nlev, cells, edges = pressure.shape[1], pressure.shape[2], velocity.shape[2]
    halo = send_cells.shape[2]
    rows, ecols = round_up(nlev, 32), round_up(edges, 128)
    hbm = pl.BlockSpec(memory_space=pltpu.HBM)
    vmem = pl.BlockSpec(memory_space=pltpu.VMEM)
    dma8 = pltpu.SemaphoreType.DMA((8,))
    args = [level_major(x) if k in (0, 1, 3, 7, 9) else x for k, x in enumerate(args)]

    def body(*refs):
        kernel(n_lat, n_lon, nlev, cells, edges, halo, *refs)

    halo_shape = pltpu.VMEM((8, rows, halo), F32)
    cell_shape = pltpu.VMEM((rows, cells), F32)
    edge_shape = pltpu.VMEM((rows, ecols), F32)
    level_shape = pltpu.VMEM((nlev, cells), F32)
    outs = pl.pallas_call(
        body,
        name="substeps",
        out_shape=(
            pltpu.VMEM(args[0].shape, F32),
            pltpu.VMEM(args[1].shape, F32),
        ),
        in_specs=[hbm] * len(args),
        out_specs=(vmem, vmem),
        scratch_shapes=[pltpu.VMEM(x.shape, x.dtype) for x in args] + [
            cell_shape, edge_shape, halo_shape, halo_shape, halo_shape, halo_shape,
            level_shape, level_shape, level_shape, cell_shape, edge_shape, cell_shape,
            dma8, dma8, dma8, dma8,
            pltpu.SemaphoreType.DMA((len(args),)),
        ],
        compiler_params=pltpu.CompilerParams(
            collective_id=0, has_side_effects=True, vmem_limit_bytes=66_000_000
        ),
    )(*args)
    outs = pl.pallas_call(
        write_out,
        name="write_out",
        out_shape=tuple(jax.ShapeDtypeStruct(x.shape, F32) for x in outs),
        in_specs=[vmem] * 2,
        out_specs=(hbm, hbm),
        scratch_shapes=[pltpu.SemaphoreType.DMA((2,))],
        compiler_params=pltpu.CompilerParams(vmem_limit_bytes=1024 * 1024),
    )(*outs)
    return tuple(level_major(x) for x in outs)


def solution(mesh):
    band = P("lat", None, "lon")
    flat = P("lat", "lon")
    return jax.shard_map(
        on_device,
        mesh=mesh,
        in_specs=(band, band, band, band, band, band, flat, band, flat, band),
        out_specs=(band, band),
        check_vma=False,
    )
```
